32 devices in a mesh: parts: 2 (over y), rows: 16 (over z, x, core).
Axes of the slice: x: 2, y: 2, z: 4, core: 2. Of those that a mesh axis runs over, the one named last changes fastest.
Arguments:
- latent: bfloat16 [4, 16, 160, 384], P('parts', 'rows'), parts along dimension 0, may hold values from -40 to 40
- conv_cache: bfloat16 [4, 16, 160, 384], P('parts', 'rows'), parts along dimension 0, may hold values from -6 to 6
- time_cache: bfloat16 [4, 16, 160, 384], P('parts', 'rows'), parts along dimension 0, may hold values from -6 to 6
- norm_gain: float32 [384], replicated, may hold values from 0.5 to 2
- norm_shift: float32 [384], replicated, may hold values from -3 to 3
- conv_weight: bfloat16 [3, 3, 3, 384, 384], replicated, may hold values from -0.0625 to 0.0625
- conv_bias: float32 [384], replicated, may hold values from -2 to 2
- time_weight: bfloat16 [3, 384, 768], replicated, may hold values from -0.1875 to 0.1875
- time_bias: float32 [768], replicated, may hold values from -2 to 2
- up_weight: bfloat16 [3, 3, 384, 192], replicated, may hold values from -0.109375 to 0.109375
- up_bias: float32 [192], replicated, may hold values from -2 to 2
Outputs:
- frames_out: bfloat16 [8, 32, 320, 192], P('parts', 'rows'), parts along dimension 0
The draws below stay inside these ranges and needn't reach their ends.
There are 2 independent parts, one for each index of `parts`. The reference program is written for one: setup_inputs(seed, part) draws one part's arguments, and reference() takes and returns one part's arrays. A program takes and returns all parts, laid end to end along the dimension named above; an argument that names none is the same for every part. Nothing has to cross between parts.
All inputs are finite; a program needn't handle non-finite values.
Results may differ from the reference program's by a relative error of at most 0.0056.
Values may be sent and summed in bfloat16 or wider, within the bound.
A program may use at most 64 MiB of HBM per device.

```python
import math
import jax
import jax.numpy as jnp
from jax import lax

C = 384
C_OUT = 192
GROUPS = 32
FRAMES = 2
WIDE = 160
HEIGHT = 16


def draw_latent(key, part):
    key_base = jax.random.fold_in(key, 11)
    key_chan = jax.random.fold_in(key, 12)
    position = jnp.arange(HEIGHT, dtype=jnp.float32) / max(HEIGHT - 1, 1)
    chan_scale = 0.3 * 10.0 ** jax.random.uniform(key_chan, (C,), jnp.float32)
    base = jnp.clip(jax.random.normal(key_base, (FRAMES, HEIGHT, WIDE, C), jnp.float32), -4.0, 4.0)
    row_scale = 0.3 * 10.0 ** position
    values = base * row_scale[None, :, None, None] * chan_scale
    return values.astype(jnp.bfloat16)


def block_levels(key, extent, shards, least, top_value):
    level = 1.0
    for dim, parts in shards:
        draws = jax.random.uniform(jax.random.fold_in(jax.random.fold_in(key, 6), dim), (parts,), jnp.float32, least / len(shards), top_value / len(shards))
        level = level * jnp.repeat(jnp.exp(draws), extent[dim] // parts).reshape((-1,) + (1,) * (len(extent) - 1 - dim))
    return level


def bell_draw(rng, extent, deviation, bound, split=(), held_as=jnp.bfloat16):
    array = deviation * jax.random.normal(rng, extent, jnp.float32)
    if split:
        array = array * block_levels(rng, extent, split, -0.22, 0.18)
    return jnp.clip(array, -bound, bound).astype(held_as)


def setup_inputs(seed: int = 0, part: int = 0) -> dict:
    key_list = jax.random.split(jax.random.key(seed), 12)
    part_keys = jax.random.split(jax.random.fold_in(key_list[11], part), 12)
    return {
        "latent": draw_latent(jax.random.fold_in(jax.random.fold_in(key_list[11], part), 71), part),
        "conv_cache": bell_draw(part_keys[1], (2, HEIGHT, WIDE, C), 1.0, 6.0, ((1, 16),)),
        "time_cache": bell_draw(part_keys[2], (2, HEIGHT, WIDE, C), 1.0, 6.0, ((1, 16),)),
        "norm_gain": jnp.clip(jnp.exp(jax.random.uniform(key_list[3], (C,), jnp.float32, math.log(0.5), math.log(2.0))), 0.5, 2.0),
        "norm_shift": bell_draw(key_list[4], (C,), 0.5, 3.0, (), jnp.float32),
        "conv_weight": bell_draw(key_list[5], (3, 3, 3, C, C), (27 * C) ** -0.5, 0.0625),
        "conv_bias": bell_draw(key_list[6], (C,), 0.3, 2.0, (), jnp.float32),
        "time_weight": bell_draw(key_list[7], (3, C, 2 * C), (3 * C) ** -0.5, 0.1875),
        "time_bias": bell_draw(key_list[8], (2 * C,), 0.3, 2.0, (), jnp.float32),
        "up_weight": bell_draw(key_list[9], (3, 3, C, C_OUT), (9 * C) ** -0.5, 0.109375),
        "up_bias": bell_draw(key_list[10], (C_OUT,), 0.3, 2.0, (), jnp.float32),
    }


EPSILON = 1e-06

def normalize(signal, norm_gain, norm_shift):
    frame_count, row_count, col_count, channels = signal.shape
    grouped = signal.reshape(frame_count, row_count, col_count, GROUPS, channels // GROUPS)
    center = lax.optimization_barrier(jnp.mean(grouped, axis=(0, 1, 2, 4), keepdims=True))
    spread = lax.optimization_barrier(jnp.mean(jnp.square(grouped - center), axis=(0, 1, 2, 4), keepdims=True))
    normed = ((grouped - center) * lax.rsqrt(spread + EPSILON)).reshape(signal.shape)
    return jax.nn.silu(normed * norm_gain + norm_shift).astype(jnp.bfloat16)

def conv_taps(padded, kernel, row_count, col_count):
    channels = padded.shape[-1]
    total = jnp.zeros((padded.shape[0] * row_count * col_count, kernel.shape[-1]), jnp.float32)
    for row_tap in range(3):
        window = jnp.concatenate([padded[:, row_tap:row_tap + row_count, col_tap:col_tap + col_count] for col_tap in range(3)], axis=-1)
        total = total + jnp.dot(window.reshape(-1, 3 * channels), kernel[row_tap].reshape(3 * channels, -1), preferred_element_type=jnp.float32)
    return total

def temporal(block, time_cache, time_weight, time_bias):
    frame_count = block.shape[0]
    channels = block.shape[-1]
    joined = jnp.concatenate([time_cache, block], axis=0)
    window = jnp.concatenate([joined[frame_tap:frame_tap + frame_count] for frame_tap in range(3)], axis=-1)
    mixed = jnp.dot(window.reshape(-1, 3 * channels), time_weight.reshape(3 * channels, -1), preferred_element_type=jnp.float32) + time_bias
    mixed = mixed.astype(jnp.bfloat16).reshape(block.shape[:-1] + (2, channels))
    return jnp.moveaxis(mixed, 3, 1).reshape((2 * frame_count,) + block.shape[1:])

def reference(latent, conv_cache, time_cache, norm_gain, norm_shift, conv_weight, conv_bias, time_weight, time_bias, up_weight, up_bias):
    frame_count, row_count, col_count, channels = latent.shape
    signal = latent.astype(jnp.float32)
    active = normalize(signal, norm_gain, norm_shift)
    joined = jnp.concatenate([conv_cache, active], axis=0)
    padded = jnp.pad(joined, ((0, 0), (1, 1), (1, 1), (0, 0)))
    summed = conv_bias + jnp.zeros((frame_count * row_count * col_count, channels), jnp.float32)
    for frame_tap in range(3):
        summed = summed + conv_taps(padded[frame_tap:frame_tap + frame_count], conv_weight[frame_tap], row_count, col_count)
    block = (signal + summed.reshape(signal.shape)).astype(jnp.bfloat16)
    doubled = temporal(block, time_cache, time_weight, time_bias)
    upsampled = jnp.repeat(jnp.repeat(doubled, 2, axis=1), 2, axis=2)
    padded_up = jnp.pad(upsampled, ((0, 0), (1, 1), (1, 1), (0, 0)))

    def one_frame(frame):
        result = conv_taps(frame[None], up_weight, 2 * row_count, 2 * col_count) + up_bias
        return result.astype(jnp.bfloat16).reshape(2 * row_count, 2 * col_count, -1)
    return lax.map(one_frame, padded_up)
```

```python
import functools

import numpy as np
import jax
import jax.numpy as jnp
from jax import lax
from jax.experimental import pallas as pl
from jax.experimental.pallas import tpu as pltpu
from jax.sharding import PartitionSpec as P

GROUPS = 32
EPSILON = 1e-06
F32 = jnp.float32
BF16 = jnp.bfloat16
MESH = pl.DeviceIdType.MESH


def dot(a, b):
    return jnp.dot(a, b, preferred_element_type=F32)


def three_columns(value):
    wide = value.shape[0]
    column = lax.broadcasted_iota(jnp.int32, value.shape, 0)
    left = jnp.where(column == 0, 0.0, pltpu.roll(value, 1, 0))
    right = jnp.where(column == wide - 1, 0.0, pltpu.roll(value, wide - 1, 0))
    return [part.astype(BF16) for part in (left, value, right)]


def kernel(
    n, lat_hbm, cc_hbm, tc_hbm, gain, shift, cw_hbm, cb, tw_hbm, tb, uw_hbm, ub, member, out,
    lat, cc, tc, cw, tw, uw, xs, acc, stats, psend, precv, blk, ul, wmid, wside, uacc, rows_out,
    in_sem, cw_sem, stat_send, stat_recv, halo_send, halo_recv,
):
    me = lax.axis_index("rows")
    frames, wide, chan = lat.shape
    c_out = uw.shape[-1]
    pad_out = wmid.shape[-1] // 2

    loads = [
        pltpu.make_async_copy(lat_hbm.at[:, 0], lat, in_sem.at[0]),
        pltpu.make_async_copy(tc_hbm.at[:, 0], tc.at[1], in_sem.at[1]),
        pltpu.make_async_copy(cc_hbm.at[:, 0], cc, in_sem.at[2]),
    ]
    for load in loads:
        load.start()
    order = (0, 2, 1)
    taps = [[], [], []]
    for a in range(3):
        for place, b in enumerate(order):
            for c in range(3):
                copy = pltpu.make_async_copy(
                    cw_hbm.at[a, b, c],
                    cw.at[a, pl.ds(c * chan, chan), pl.ds(place * chan, chan)],
                    cw_sem.at[a, place * 3 + c],
                )
                copy.start()
                taps[a].append(copy)
    up_load = pltpu.make_async_copy(uw_hbm, uw, in_sem.at[3])
    up_load.start()
    time_load = pltpu.make_async_copy(tw_hbm, tw, in_sem.at[4])
    time_load.start()

    barrier = pltpu.get_barrier_semaphore()

    @pl.loop(1, n)
    def _(k):
        pl.semaphore_signal(
            barrier, inc=1, device_id={"rows": lax.rem(me + k, n)}, device_id_type=MESH
        )

    loads[0].wait()
    signal = lat[...].astype(F32).reshape(frames * wide, chan)
    entries = float(frames * wide)
    local_sum = jnp.sum(signal, axis=0, keepdims=True)
    off = signal - local_sum / entries
    stats[me] = jnp.concatenate([local_sum, jnp.sum(off * off, axis=0, keepdims=True)], axis=0)
    pl.semaphore_wait(barrier, n - 1)

    def stat_copy(k):
        return pltpu.make_async_remote_copy(
            src_ref=stats.at[me], dst_ref=stats.at[me],
            send_sem=stat_send.at[k], recv_sem=stat_recv.at[k],
            device_id={"rows": lax.rem(me + k, n)}, device_id_type=MESH,
        )

    @pl.loop(1, n)
    def _(k):
        stat_copy(k).start()

    def to_after(src, dst, i):
        return pltpu.make_async_remote_copy(
            src_ref=src, dst_ref=dst, send_sem=halo_send.at[i], recv_sem=halo_recv.at[i],
            device_id={"rows": lax.rem(me + 1, n)}, device_id_type=MESH,
        )

    def to_before(src, dst, i):
        return pltpu.make_async_remote_copy(
            src_ref=src, dst_ref=dst, send_sem=halo_send.at[i], recv_sem=halo_recv.at[i],
            device_id={"rows": lax.rem(me + n - 1, n)}, device_id_type=MESH,
        )

    has_before = me > 0
    has_after = me < n - 1

    def exchange(up, down):
        @pl.when(has_after)
        def _():
            up.start()

        @pl.when(has_before)
        def _():
            down.start()

    def arrive(up, down):
        @pl.when(has_before)
        def _():
            up.wait_recv()

        @pl.when(has_after)
        def _():
            down.wait_recv()

    def sent(up, down):
        @pl.when(has_after)
        def _():
            up.wait_send()

        @pl.when(has_before)
        def _():
            down.wait_send()

    loads[1].wait()
    time_up = to_after(tc.at[1], tc.at[0], 0)
    time_down = to_before(tc.at[1], tc.at[2], 1)
    exchange(time_up, time_down)

    @pl.when(me == 0)
    def _():
        tc[0] = jnp.zeros_like(tc[0])
        precv[0] = jnp.zeros_like(precv[0])
        blk[0] = jnp.zeros_like(blk[0])

    @pl.when(me == n - 1)
    def _():
        tc[2] = jnp.zeros_like(tc[2])
        precv[1] = jnp.zeros_like(precv[1])
        blk[2] = jnp.zeros_like(blk[2])

    def put_three(ref, start, value):
        for i, part in enumerate(three_columns(value)):
            ref[pl.ds(start, wide), pl.ds(i * chan, chan)] = part

    loads[2].wait()
    for f in range(2):
        put_three(xs, f * wide, cc[f].astype(F32))
    for copy in taps[0]:
        copy.wait()
    acc[...] = dot(xs[pl.ds(0, 2 * wide), :], cw[0])
    for copy in taps[1]:
        copy.wait()
    acc[pl.ds(0, wide), :] += dot(xs[pl.ds(wide, wide), :], cw[1])

    up_load.wait()
    wmid[...] = jnp.zeros_like(wmid)
    wside[...] = jnp.zeros_like(wside)
    w = [[uw[b, c].astype(F32) for c in range(3)] for b in range(3)]
    row_mid = ([w[1][c] + w[2][c] for c in range(3)], [w[0][c] + w[1][c] for c in range(3)])
    row_side = (w[0], w[2])
    for row in range(2):
        for dest, part, base in ((wmid, row_mid[row], row * pad_out), (wside, row_side[row], None)):
            pairs = ((part[0], part[1] + part[2]), (part[0] + part[1], part[2]))
            for q in range(2):
                for j in range(2):
                    rows = pl.ds(j * chan, chan)
                    value = pairs[q][j].astype(BF16)
                    if base is None:
                        dest[row, q, rows, pl.ds(0, c_out)] = value
                    else:
                        dest[q, rows, pl.ds(base, c_out)] = value

    @pl.loop(1, n)
    def _(k):
        stat_copy(k).wait()

    total_entries = entries * n * (chan // GROUPS)
    spread_over = member[...].astype(F32)

    def per_group(value):
        value = jnp.broadcast_to(value, (8, chan))
        got = jnp.dot(
            value, spread_over, preferred_element_type=F32, precision=lax.Precision.HIGHEST
        )
        return got[0:1]

    every = stats[...]
    sums = every[:, 0]
    center = per_group(jnp.sum(sums, axis=0, keepdims=True)) / total_entries
    gap = sums / entries - center
    squares = jnp.sum(every[:, 1] + entries * gap * gap, axis=0, keepdims=True)
    spread = per_group(squares) / total_entries
    factor = lax.rsqrt(spread + EPSILON) * gain[...]
    for f in range(frames):
        value = (lat[f].astype(F32) - center) * factor + shift[...]
        active = value / (1.0 + jnp.exp(-value))
        put_three(xs, (2 + f) * wide, active.astype(BF16).astype(F32))

    for copy in taps[2]:
        copy.wait()
    sides = pl.ds(0, 2 * chan)
    middle = pl.ds(2 * chan, chan)
    second = pl.ds(wide, wide)
    first = pl.ds(0, wide)
    acc[second, sides] += dot(xs[pl.ds(2 * wide, wide), :], cw[1, :, sides])
    edge = acc[:, sides] + dot(xs[pl.ds(2 * wide, 2 * wide), :], cw[2, :, sides])
    psend[0] = edge[:, :chan].astype(BF16)
    psend[1] = edge[:, chan:].astype(BF16)
    part_up = to_after(psend.at[0], precv.at[0], 2)
    part_down = to_before(psend.at[1], precv.at[1], 3)
    exchange(part_up, part_down)
    acc[second, middle] += dot(xs[pl.ds(2 * wide, wide), :], cw[1, :, middle])
    acc[:, middle] += dot(xs[pl.ds(2 * wide, 2 * wide), :], cw[2, :, middle])
    arrive(part_up, part_down)
    summed = acc[:, middle] + precv[0].astype(F32) + precv[1].astype(F32) + cb[...]
    blk[1] = (lat[...].astype(F32).reshape(frames * wide, chan) + summed).astype(BF16)
    block_up = to_after(blk.at[1], blk.at[0], 4)
    block_down = to_before(blk.at[1], blk.at[2], 5)
    exchange(block_up, block_down)

    def temporal(row, keep):
        for t in range(frames):
            window = []
            for a in range(3):
                s = t + a
                window.append(tc[row, s] if s < 2 else blk[row, pl.ds((s - 2) * wide, wide), :])
            mixed = dot(jnp.concatenate(window, axis=-1), tw[...]) + tb[...]
            mixed = mixed.astype(BF16).astype(F32)
            if keep is not None:
                mixed = jnp.where(keep, mixed, 0.0)
            for k in range(2):
                put_three(
                    ul.at[row], (2 * t + k) * wide, mixed[:, k * chan : (k + 1) * chan]
                )

    time_load.wait()
    temporal(1, None)
    for q in range(2):
        uacc[q] = dot(ul[1, :, pl.ds(q * chan, 2 * chan)], wmid[q])
    arrive(time_up, time_down)
    arrive(block_up, block_down)
    for row, p, keep in ((0, 0, has_before), (2, 1, has_after)):
        temporal(row, keep)
        for q in range(2):
            columns = pl.ds(p * pad_out, pad_out)
            result = uacc[q, :, columns] + dot(ul[row, :, pl.ds(q * chan, 2 * chan)], wside[p, q])
            result = result + ub[...]
            uacc[q, :, columns] = result
        for f in range(2 * frames):
            for half in range(pad_out // 128):
                lanes = min(128, c_out - half * 128)
                for q in range(2):
                    rows_out[half, pl.ds(q, wide, stride=2), :] = uacc[
                        q, pl.ds(f * wide, wide), pl.ds(p * pad_out + half * 128, 128)
                    ]
                out[f, p, :, pl.ds(half * 128, lanes)] = rows_out[half][:, :lanes].astype(BF16)
    sent(time_up, time_down)
    sent(part_up, part_down)
    sent(block_up, block_down)


def on_device(
    latent, conv_cache, time_cache, norm_gain, norm_shift, conv_weight, conv_bias,
    time_weight, time_bias, up_weight, up_bias,
):
    n = lax.axis_size("rows")
    frames, row_count, wide, chan = latent.shape
    assert row_count == 1
    c_out = up_weight.shape[-1]
    pad_out = -(-c_out // 128) * 128
    width = chan // GROUPS
    member = np.arange(chan) // width
    member = jnp.asarray(member[:, None] == member[None, :], dtype=BF16)
    hbm = pl.BlockSpec(memory_space=pl.ANY)
    vmem = pl.BlockSpec(memory_space=pltpu.VMEM)
    dma = pltpu.SemaphoreType.DMA
    out = pl.pallas_call(
        functools.partial(kernel, n),
        out_shape=jax.ShapeDtypeStruct((2 * frames, 2, 2 * wide, c_out), BF16),
        in_specs=[hbm, hbm, hbm, vmem, vmem, hbm, vmem, hbm, vmem, hbm, vmem, vmem],
        out_specs=vmem,
        scratch_shapes=[
            pltpu.VMEM((frames, wide, chan), BF16),
            pltpu.VMEM((2, wide, chan), BF16),
            pltpu.VMEM((3, 2, wide, chan), BF16),
            pltpu.VMEM((3, 3 * chan, 3 * chan), BF16),
            pltpu.VMEM((3 * chan, 2 * chan), BF16),
            pltpu.VMEM((3, 3, chan, c_out), BF16),
            pltpu.VMEM(((2 + frames) * wide, 3 * chan), BF16),
            pltpu.VMEM((frames * wide, 3 * chan), F32),
            pltpu.VMEM((n, 2, chan), F32),
            pltpu.VMEM((2, frames * wide, chan), BF16),
            pltpu.VMEM((2, frames * wide, chan), BF16),
            pltpu.VMEM((3, frames * wide, chan), BF16),
            pltpu.VMEM((3, 2 * frames * wide, 3 * chan), BF16),
            pltpu.VMEM((2, 2 * chan, 2 * pad_out), BF16),
            pltpu.VMEM((2, 2, 2 * chan, pad_out), BF16),
            pltpu.VMEM((2, 2 * frames * wide, 2 * pad_out), F32),
            pltpu.VMEM((pad_out // 128, 2 * wide, 128), F32),
            dma((5,)),
            dma((3, 9)),
            dma((n,)),
            dma((n,)),
            dma((6,)),
            dma((6,)),
        ],
        compiler_params=pltpu.CompilerParams(
            collective_id=0, has_side_effects=True, vmem_limit_bytes=60000 * 1024
        ),
    )(
        latent, conv_cache, time_cache, norm_gain[None], norm_shift[None], conv_weight,
        conv_bias[None], time_weight.reshape(3 * chan, 2 * chan), time_bias[None], up_weight,
        jnp.pad(up_bias, (0, pad_out - c_out))[None], member,
    )
    return out


def solution(mesh):
    split = P("parts", "rows", None, None)
    return jax.shard_map(
        on_device,
        mesh=mesh,
        in_specs=(split, split, split) + (P(),) * 8,
        out_specs=split,
        check_vma=False,
    )
```

```python
import functools

import numpy as np
import jax
import jax.numpy as jnp
from jax import lax
from jax.experimental import pallas as pl
from jax.experimental.pallas import tpu as pltpu
from jax.sharding import PartitionSpec as P

GROUPS = 32
EPSILON = 1e-06
F32 = jnp.float32
BF16 = jnp.bfloat16
MESH = pl.DeviceIdType.MESH


def dot(a, b):
    return jnp.dot(a, b, preferred_element_type=F32)


def dot_turned(a, b):
    return lax.dot_general(a, b, (((1,), (1,)), ((), ())), preferred_element_type=F32)


def three_columns(value):
    wide = value.shape[0]
    column = lax.broadcasted_iota(jnp.int32, value.shape, 0)
    left = jnp.where(column == 0, 0.0, pltpu.roll(value, 1, 0))
    right = jnp.where(column == wide - 1, 0.0, pltpu.roll(value, wide - 1, 0))
    return [part.astype(BF16) for part in (left, value, right)]


def kernel(
    n, lat_hbm, cc_hbm, tc_hbm, gain, shift, cw_hbm, cb, tw_hbm, tb, uw_hbm, ub, member_hbm, out,
    lat, cc, tc, cw, tw, uw, xs, acc, stats, psend, precv, blk, ul, wmid, wside, uacc, rows_out, member,
    in_sem, cw_sem, stat_send, stat_recv, halo_send, halo_recv,
):
    me = lax.axis_index("rows")
    frames, wide, chan = lat.shape
    c_out = uw.shape[2]
    pad_out = wside.shape[2]

    loads = [
        pltpu.make_async_copy(lat_hbm.at[:, 0], lat, in_sem.at[0]),
        pltpu.make_async_copy(tc_hbm.at[:, 0], tc.at[1], in_sem.at[1]),
        pltpu.make_async_copy(cc_hbm.at[:, 0], cc, in_sem.at[2]),
    ]
    for load in loads:
        load.start()
    order = (0, 2, 1)
    taps = [[], [], []]
    for a in range(3):
        for place, b in enumerate(order):
            for c in range(3):
                copy = pltpu.make_async_copy(
                    cw_hbm.at[a, b, c],
                    cw.at[a, pl.ds(c * chan, chan), pl.ds(place * chan, chan)],
                    cw_sem.at[a, place * 3 + c],
                )
                copy.start()
                taps[a].append(copy)
    up_load = pltpu.make_async_copy(uw_hbm, uw, in_sem.at[3])
    up_load.start()
    time_load = pltpu.make_async_copy(tw_hbm, tw, in_sem.at[4])
    time_load.start()
    member_load = pltpu.make_async_copy(member_hbm, member, in_sem.at[5])
    member_load.start()

    barrier = pltpu.get_barrier_semaphore()

    @pl.loop(1, n)
    def _(k):
        pl.semaphore_signal(
            barrier, inc=1, device_id={"rows": lax.rem(me + k, n)}, device_id_type=MESH
        )

    loads[0].wait()
    signal = lat[...].astype(F32).reshape(frames * wide, chan)
    entries = float(frames * wide)
    local_sum = jnp.sum(signal, axis=0, keepdims=True)
    off = signal - local_sum / entries
    stats[me] = jnp.concatenate([local_sum, jnp.sum(off * off, axis=0, keepdims=True)], axis=0)
    pl.semaphore_wait(barrier, n - 1)

    def stat_copy(k):
        return pltpu.make_async_remote_copy(
            src_ref=stats.at[me], dst_ref=stats.at[me],
            send_sem=stat_send.at[k], recv_sem=stat_recv.at[k],
            device_id={"rows": lax.rem(me + k, n)}, device_id_type=MESH,
        )

    @pl.loop(1, n)
    def _(k):
        stat_copy(k).start()

    def to_after(src, dst, i):
        return pltpu.make_async_remote_copy(
            src_ref=src, dst_ref=dst, send_sem=halo_send.at[i], recv_sem=halo_recv.at[i],
            device_id={"rows": lax.rem(me + 1, n)}, device_id_type=MESH,
        )

    def to_before(src, dst, i):
        return pltpu.make_async_remote_copy(
            src_ref=src, dst_ref=dst, send_sem=halo_send.at[i], recv_sem=halo_recv.at[i],
            device_id={"rows": lax.rem(me + n - 1, n)}, device_id_type=MESH,
        )

    has_before = me > 0
    has_after = me < n - 1

    def exchange(up, down):
        @pl.when(has_after)
        def _():
            up.start()

        @pl.when(has_before)
        def _():
            down.start()

    def arrive(up, down):
        @pl.when(has_before)
        def _():
            up.wait_recv()

        @pl.when(has_after)
        def _():
            down.wait_recv()

    def sent(up, down):
        @pl.when(has_after)
        def _():
            up.wait_send()

        @pl.when(has_before)
        def _():
            down.wait_send()

    loads[1].wait()
    time_up = to_after(tc.at[1], tc.at[0], 0)
    time_down = to_before(tc.at[1], tc.at[2], 1)
    exchange(time_up, time_down)

    @pl.when(me == 0)
    def _():
        tc[0] = jnp.zeros_like(tc[0])
        precv[0] = jnp.zeros_like(precv[0])
        blk[0] = jnp.zeros_like(blk[0])

    @pl.when(me == n - 1)
    def _():
        tc[2] = jnp.zeros_like(tc[2])
        precv[1] = jnp.zeros_like(precv[1])
        blk[2] = jnp.zeros_like(blk[2])

    def put_three(ref, start, value):
        for i, part in enumerate(three_columns(value)):
            ref[pl.ds(start, wide), pl.ds(i * chan, chan)] = part

    loads[2].wait()
    for f in range(2):
        put_three(xs, f * wide, cc[f].astype(F32))
    for copy in taps[0]:
        copy.wait()
    acc[...] = dot(xs[pl.ds(0, 2 * wide), :], cw[0])
    for copy in taps[1]:
        copy.wait()
    acc[pl.ds(0, wide), :] += dot(xs[pl.ds(wide, wide), :], cw[1])

    up_load.wait()
    wmid[...] = jnp.zeros_like(wmid)
    wside[...] = jnp.zeros_like(wside)
    w = [[uw[b, c].astype(F32) for c in range(3)] for b in range(3)]
    row_mid = ([w[1][c] + w[2][c] for c in range(3)], [w[0][c] + w[1][c] for c in range(3)])
    row_side = (w[0], w[2])
    for row in range(2):
        for dest, part in ((wmid, row_mid[row]), (wside, row_side[row])):
            pairs = ((part[0], part[1] + part[2]), (part[0] + part[1], part[2]))
            for q in range(2):
                for j in range(2):
                    value = pairs[q][j].astype(BF16)
                    lanes = pl.ds(j * chan, chan)
                    if dest is wmid:
                        dest[q, pl.ds(row * pad_out, c_out), lanes] = value
                    else:
                        dest[row, q, pl.ds(0, c_out), lanes] = value

    @pl.loop(1, n)
    def _(k):
        stat_copy(k).wait()

    total_entries = entries * n * (chan // GROUPS)
    member_load.wait()
    spread_over = member[...].astype(F32)

    def per_group(value):
        value = jnp.broadcast_to(value, (8, chan))
        got = jnp.dot(
            value, spread_over, preferred_element_type=F32, precision=lax.Precision.HIGHEST
        )
        return got[0:1]

    every = stats[...]
    sums = every[:, 0]
    center = per_group(jnp.sum(sums, axis=0, keepdims=True)) / total_entries
    gap = sums / entries - center
    squares = jnp.sum(every[:, 1] + entries * gap * gap, axis=0, keepdims=True)
    spread = per_group(squares) / total_entries
    factor = lax.rsqrt(spread + EPSILON) * gain[...][None]
    for f in range(frames):
        value = (lat[f].astype(F32) - center) * factor + shift[...][None]
        active = value / (1.0 + jnp.exp(-value))
        put_three(xs, (2 + f) * wide, active.astype(BF16).astype(F32))

    for copy in taps[2]:
        copy.wait()
    sides = pl.ds(0, 2 * chan)
    middle = pl.ds(2 * chan, chan)
    second = pl.ds(wide, wide)
    first = pl.ds(0, wide)
    acc[second, sides] += dot(xs[pl.ds(2 * wide, wide), :], cw[1, :, sides])
    edge = acc[:, sides] + dot(xs[pl.ds(2 * wide, 2 * wide), :], cw[2, :, sides])
    psend[0] = edge[:, :chan].astype(BF16)
    psend[1] = edge[:, chan:].astype(BF16)
    part_up = to_after(psend.at[0], precv.at[0], 2)
    part_down = to_before(psend.at[1], precv.at[1], 3)
    exchange(part_up, part_down)
    acc[second, middle] += dot(xs[pl.ds(2 * wide, wide), :], cw[1, :, middle])
    acc[:, middle] += dot(xs[pl.ds(2 * wide, 2 * wide), :], cw[2, :, middle])
    arrive(part_up, part_down)
    summed = acc[:, middle] + precv[0].astype(F32) + precv[1].astype(F32) + cb[...][None]
    blk[1] = (lat[...].astype(F32).reshape(frames * wide, chan) + summed).astype(BF16)
    block_up = to_after(blk.at[1], blk.at[0], 4)
    block_down = to_before(blk.at[1], blk.at[2], 5)
    exchange(block_up, block_down)

    def temporal(row, keep):
        for t in range(frames):
            window = []
            for a in range(3):
                s = t + a
                window.append(tc[row, s] if s < 2 else blk[row, pl.ds((s - 2) * wide, wide), :])
            mixed = dot(jnp.concatenate(window, axis=-1), tw[...]) + tb[...][None]
            mixed = mixed.astype(BF16).astype(F32)
            if keep is not None:
                mixed = jnp.where(keep, mixed, 0.0)
            for k in range(2):
                put_three(
                    ul.at[row], (2 * t + k) * wide, mixed[:, k * chan : (k + 1) * chan]
                )

    time_load.wait()
    temporal(1, None)
    for q in range(2):
        uacc[q] = dot_turned(ul[1, :, pl.ds(q * chan, 2 * chan)], wmid[q])
    arrive(time_up, time_down)
    arrive(block_up, block_down)
    for row, p, keep in ((0, 0, has_before), (2, 1, has_after)):
        temporal(row, keep)
        for q in range(2):
            columns = pl.ds(p * pad_out, pad_out)
            result = uacc[q, :, columns] + dot_turned(
                ul[row, :, pl.ds(q * chan, 2 * chan)], wside[p, q]
            )
            uacc[q, :, columns] = result
        for f in range(2 * frames):
            for half in range(pad_out // 128):
                lanes = min(128, c_out - half * 128)
                for q in range(2):
                    rows_out[half, pl.ds(q, wide, stride=2), :] = uacc[
                        q, pl.ds(f * wide, wide), pl.ds(p * pad_out + half * 128, 128)
                    ]
                out[f, p, :, pl.ds(half * 128, lanes)] = (
                    rows_out[half][:, :lanes] + ub[...][None, half * 128 : half * 128 + lanes]
                ).astype(BF16)
    sent(time_up, time_down)
    sent(part_up, part_down)
    sent(block_up, block_down)


def on_device(
    latent, conv_cache, time_cache, norm_gain, norm_shift, conv_weight, conv_bias,
    time_weight, time_bias, up_weight, up_bias,
):
    n = lax.axis_size("rows")
    frames, row_count, wide, chan = latent.shape
    assert row_count == 1
    c_out = up_weight.shape[-1]
    pad_out = -(-c_out // 128) * 128
    width = chan // GROUPS
    member = np.arange(chan) // width
    member = jnp.asarray(member[:, None] == member[None, :], dtype=BF16)
    hbm = pl.BlockSpec(memory_space=pl.ANY)
    vmem = pl.BlockSpec(memory_space=pltpu.VMEM)
    dma = pltpu.SemaphoreType.DMA
    out = pl.pallas_call(
        functools.partial(kernel, n),
        out_shape=jax.ShapeDtypeStruct((2 * frames, 2, 2 * wide, c_out), BF16),
        in_specs=[hbm, hbm, hbm, vmem, vmem, hbm, vmem, hbm, vmem, hbm, vmem, hbm],
        out_specs=vmem,
        scratch_shapes=[
            pltpu.VMEM((frames, wide, chan), BF16),
            pltpu.VMEM((2, wide, chan), BF16),
            pltpu.VMEM((3, 2, wide, chan), BF16),
            pltpu.VMEM((3, 3 * chan, 3 * chan), BF16),
            pltpu.VMEM((3 * chan, 2 * chan), BF16),
            pltpu.VMEM((3, 3, c_out, chan), BF16),
            pltpu.VMEM(((2 + frames) * wide, 3 * chan), BF16),
            pltpu.VMEM((frames * wide, 3 * chan), F32),
            pltpu.VMEM((n, 2, chan), F32),
            pltpu.VMEM((2, frames * wide, chan), BF16),
            pltpu.VMEM((2, frames * wide, chan), BF16),
            pltpu.VMEM((3, frames * wide, chan), BF16),
            pltpu.VMEM((3, 2 * frames * wide, 3 * chan), BF16),
            pltpu.VMEM((2, 2 * pad_out, 2 * chan), BF16),
            pltpu.VMEM((2, 2, pad_out, 2 * chan), BF16),
            pltpu.VMEM((2, 2 * frames * wide, 2 * pad_out), F32),
            pltpu.VMEM((pad_out // 128, 2 * wide, 128), F32),
            pltpu.VMEM((chan, chan), BF16),
            dma((6,)),
            dma((3, 9)),
            dma((n,)),
            dma((n,)),
            dma((6,)),
            dma((6,)),
        ],
        compiler_params=pltpu.CompilerParams(
            collective_id=0, has_side_effects=True, vmem_limit_bytes=60000 * 1024
        ),
    )(
        latent, conv_cache, time_cache, norm_gain, norm_shift, conv_weight, conv_bias,
        time_weight.reshape(3 * chan, 2 * chan), time_bias, jnp.swapaxes(up_weight, 2, 3),
        up_bias, member,
    )
    return out


def solution(mesh):
    split = P("parts", "rows", None, None)
    return jax.shard_map(
        on_device,
        mesh=mesh,
        in_specs=(split, split, split) + (P(),) * 8,
        out_specs=split,
        check_vma=False,
    )
```

```python
import functools

import numpy as np
import jax
import jax.numpy as jnp
from jax import lax
from jax.experimental import pallas as pl
from jax.experimental.pallas import tpu as pltpu
from jax.sharding import PartitionSpec as P

GROUPS = 32
EPSILON = 1e-06
F32 = jnp.float32
BF16 = jnp.bfloat16
MESH = pl.DeviceIdType.MESH


def dot(a, b):
    return jnp.dot(a, b, preferred_element_type=F32)


def dot_turned(a, b):
    return lax.dot_general(a, b, (((1,), (1,)), ((), ())), preferred_element_type=F32)


def three_columns(value):
    wide = value.shape[0]
    column = lax.broadcasted_iota(jnp.int32, value.shape, 0)
    left = jnp.where(column == 0, 0.0, pltpu.roll(value, 1, 0))
    right = jnp.where(column == wide - 1, 0.0, pltpu.roll(value, wide - 1, 0))
    return [part.astype(BF16) for part in (left, value, right)]


def kernel(
    n, lat_hbm, cc_hbm, tc_hbm, gain, shift, cw_hbm, cb, tw_hbm, tb, uw_hbm, ub, member_hbm, out_hbm,
    lat, cc, tc, cw, tw, uw, xs, acc, stats, psend, precv, blk, ul, wmid, wside, uacc, rows_out, member, out,
    in_sem, cw_sem, stat_send, stat_recv, halo_send, halo_recv, out_sem,
):
    me = lax.axis_index("rows")
    frames, wide, chan = lat.shape
    c_out = uw.shape[2]
    pad_out = wside.shape[2]

    loads = [
        pltpu.make_async_copy(lat_hbm.at[:, 0], lat, in_sem.at[0]),
        pltpu.make_async_copy(tc_hbm.at[:, 0], tc.at[1], in_sem.at[1]),
        pltpu.make_async_copy(cc_hbm.at[:, 0], cc, in_sem.at[2]),
    ]
    for load in loads:
        load.start()
    order = (0, 2, 1)
    taps = [[], [], []]
    for a in range(3):
        for place, b in enumerate(order):
            for c in range(3):
                copy = pltpu.make_async_copy(
                    cw_hbm.at[a, b, c],
                    cw.at[a, pl.ds(c * chan, chan), pl.ds(place * chan, chan)],
                    cw_sem.at[a, place * 3 + c],
                )
                copy.start()
                taps[a].append(copy)
    up_load = pltpu.make_async_copy(uw_hbm, uw, in_sem.at[3])
    up_load.start()
    time_load = pltpu.make_async_copy(tw_hbm, tw, in_sem.at[4])
    time_load.start()
    member_load = pltpu.make_async_copy(member_hbm, member, in_sem.at[5])
    member_load.start()

    barrier = pltpu.get_barrier_semaphore()

    @pl.loop(1, n)
    def _(k):
        pl.semaphore_signal(
            barrier, inc=1, device_id={"rows": lax.rem(me + k, n)}, device_id_type=MESH
        )

    loads[0].wait()
    signal = lat[...].astype(F32).reshape(frames * wide, chan)
    entries = float(frames * wide)
    local_sum = jnp.sum(signal, axis=0, keepdims=True)
    off = signal - local_sum / entries
    stats[me] = jnp.concatenate([local_sum, jnp.sum(off * off, axis=0, keepdims=True)], axis=0)
    pl.semaphore_wait(barrier, n - 1)

    def stat_copy(k):
        return pltpu.make_async_remote_copy(
            src_ref=stats.at[me], dst_ref=stats.at[me],
            send_sem=stat_send.at[k], recv_sem=stat_recv.at[k],
            device_id={"rows": lax.rem(me + k, n)}, device_id_type=MESH,
        )

    @pl.loop(1, n)
    def _(k):
        stat_copy(k).start()

    def to_after(src, dst, i):
        return pltpu.make_async_remote_copy(
            src_ref=src, dst_ref=dst, send_sem=halo_send.at[i], recv_sem=halo_recv.at[i],
            device_id={"rows": lax.rem(me + 1, n)}, device_id_type=MESH,
        )

    def to_before(src, dst, i):
        return pltpu.make_async_remote_copy(
            src_ref=src, dst_ref=dst, send_sem=halo_send.at[i], recv_sem=halo_recv.at[i],
            device_id={"rows": lax.rem(me + n - 1, n)}, device_id_type=MESH,
        )

    has_before = me > 0
    has_after = me < n - 1

    def exchange(up, down):
        @pl.when(has_after)
        def _():
            up.start()

        @pl.when(has_before)
        def _():
            down.start()

    def arrive(up, down):
        @pl.when(has_before)
        def _():
            up.wait_recv()

        @pl.when(has_after)
        def _():
            down.wait_recv()

    def sent(up, down):
        @pl.when(has_after)
        def _():
            up.wait_send()

        @pl.when(has_before)
        def _():
            down.wait_send()

    loads[1].wait()
    time_up = to_after(tc.at[1], tc.at[0], 0)
    time_down = to_before(tc.at[1], tc.at[2], 1)
    exchange(time_up, time_down)

    @pl.when(me == 0)
    def _():
        tc[0] = jnp.zeros_like(tc[0])
        precv[0] = jnp.zeros_like(precv[0])
        blk[0] = jnp.zeros_like(blk[0])

    @pl.when(me == n - 1)
    def _():
        tc[2] = jnp.zeros_like(tc[2])
        precv[1] = jnp.zeros_like(precv[1])
        blk[2] = jnp.zeros_like(blk[2])

    def put_three(ref, start, value):
        for i, part in enumerate(three_columns(value)):
            ref[pl.ds(start, wide), pl.ds(i * chan, chan)] = part

    loads[2].wait()
    for f in range(2):
        put_three(xs, f * wide, cc[f].astype(F32))
    for copy in taps[0]:
        copy.wait()
    acc[...] = dot(xs[pl.ds(0, 2 * wide), :], cw[0])
    for copy in taps[1]:
        copy.wait()
    acc[pl.ds(0, wide), :] += dot(xs[pl.ds(wide, wide), :], cw[1])

    up_load.wait()
    wmid[...] = jnp.zeros_like(wmid)
    wside[...] = jnp.zeros_like(wside)
    w = [[uw[b, c].astype(F32) for c in range(3)] for b in range(3)]
    row_mid = ([w[1][c] + w[2][c] for c in range(3)], [w[0][c] + w[1][c] for c in range(3)])
    row_side = (w[0], w[2])
    for row in range(2):
        for dest, part in ((wmid, row_mid[row]), (wside, row_side[row])):
            pairs = ((part[0], part[1] + part[2]), (part[0] + part[1], part[2]))
            for q in range(2):
                for j in range(2):
                    value = pairs[q][j].astype(BF16)
                    lanes = pl.ds(j * chan, chan)
                    if dest is wmid:
                        dest[q, pl.ds(row * pad_out, c_out), lanes] = value
                    else:
                        dest[row, q, pl.ds(0, c_out), lanes] = value

    @pl.loop(1, n)
    def _(k):
        stat_copy(k).wait()

    total_entries = entries * n * (chan // GROUPS)
    member_load.wait()
    spread_over = member[...].astype(F32)

    def per_group(value):
        value = jnp.broadcast_to(value, (8, chan))
        got = jnp.dot(
            value, spread_over, preferred_element_type=F32, precision=lax.Precision.HIGHEST
        )
        return got[0:1]

    every = stats[...]
    sums = every[:, 0]
    center = per_group(jnp.sum(sums, axis=0, keepdims=True)) / total_entries
    gap = sums / entries - center
    squares = jnp.sum(every[:, 1] + entries * gap * gap, axis=0, keepdims=True)
    spread = per_group(squares) / total_entries
    factor = lax.rsqrt(spread + EPSILON) * gain[...][None]

    def activate(f):
        value = (lat[f].astype(F32) - center) * factor + shift[...][None]
        active = value / (1.0 + jnp.exp(-value))
        put_three(xs, (2 + f) * wide, active.astype(BF16).astype(F32))

    for copy in taps[2]:
        copy.wait()
    sides = pl.ds(0, 2 * chan)
    middle = pl.ds(2 * chan, chan)

    def frame(t):
        return pl.ds(t * wide, wide)

    parts, blocks = [], []
    for t in range(frames):
        activate(t)
        edge = acc[frame(t), sides]
        for s in range(t + 1):
            edge = edge + dot(xs[frame(2 + s), :], cw[2 + s - t, :, sides])
        psend[0, frame(t), :] = edge[:, :chan].astype(BF16)
        psend[1, frame(t), :] = edge[:, chan:].astype(BF16)
        parts.append((
            to_after(psend.at[0, frame(t)], precv.at[0, frame(t)], 2 + 2 * t),
            to_before(psend.at[1, frame(t)], precv.at[1, frame(t)], 3 + 2 * t),
        ))
        exchange(*parts[t])
    acc[frame(1), middle] += dot(xs[frame(2), :], cw[1, :, middle])
    acc[:, middle] += dot(xs[pl.ds(2 * wide, 2 * wide), :], cw[2, :, middle])
    time_load.wait()

    def temporal(row, t, keep):
        window = []
        for a in range(3):
            s = t + a
            window.append(tc[row, s] if s < 2 else blk[row, frame(s - 2), :])
        mixed = dot(jnp.concatenate(window, axis=-1), tw[...]) + tb[...][None]
        mixed = mixed.astype(BF16).astype(F32)
        if keep is not None:
            mixed = jnp.where(keep, mixed, 0.0)
        for k in range(2):
            put_three(ul.at[row], (2 * t + k) * wide, mixed[:, k * chan : (k + 1) * chan])

    def both(t):
        return pl.ds(2 * t * wide, 2 * wide)

    base = 2 + 2 * frames
    for t in range(frames):
        arrive(*parts[t])
        summed = (
            acc[frame(t), middle] + precv[0, frame(t), :].astype(F32)
            + precv[1, frame(t), :].astype(F32) + cb[...][None]
        )
        blk[1, frame(t), :] = (lat[t].astype(F32) + summed).astype(BF16)
        blocks.append((
            to_after(blk.at[1, frame(t)], blk.at[0, frame(t)], base + 2 * t),
            to_before(blk.at[1, frame(t)], blk.at[2, frame(t)], base + 2 * t + 1),
        ))
        exchange(*blocks[t])
        temporal(1, t, None)
        for q in range(2):
            got = dot_turned(ul[1, both(t), pl.ds(q * chan, 2 * chan)], wmid[q])
            for p in range(2):
                uacc[p, q, both(t), :] = got[:, p * pad_out : (p + 1) * pad_out]
    arrive(time_up, time_down)

    even = lax.rem(me, 2) == 0
    near = jnp.where(even, 1, 0)
    near_keep = jnp.where(even, has_after, has_before)
    far_keep = jnp.where(even, has_before, has_after)

    def halo(t, p, keep):
        row = 2 * p
        temporal(row, t, keep)
        for q in range(2):
            uacc[p, q, both(t), :] += dot_turned(
                ul[row, both(t), pl.ds(q * chan, 2 * chan)], wside[p, q]
            )
        for f in (2 * t, 2 * t + 1):
            for half in range(pad_out // 128):
                lanes = min(128, c_out - half * 128)
                for q in range(2):
                    rows_out[half, pl.ds(q, wide, stride=2), :] = uacc[
                        p, q, frame(f), pl.ds(half * 128, 128)
                    ]
                out[f, p, :, pl.ds(half * 128, lanes)] = (
                    rows_out[half][:, :lanes] + ub[...][None, half * 128 : half * 128 + lanes]
                ).astype(BF16)
            leave(f, p, keep is near_keep).start()

    def leave(f, p, first):
        return pltpu.make_async_copy(
            out.at[f, p], out_hbm.at[f, p], out_sem.at[f, 0 if first else 1]
        )

    for t in range(frames):
        up, down = blocks[t]

        @pl.when(even & has_after)
        def _():
            down.wait_recv()

        @pl.when(jnp.logical_not(even) & has_before)
        def _():
            up.wait_recv()

        halo(t, near, near_keep)

        @pl.when(even & has_before)
        def _():
            up.wait_recv()

        @pl.when(jnp.logical_not(even) & has_after)
        def _():
            down.wait_recv()

        halo(t, 1 - near, far_keep)
    for f in range(2 * frames):
        leave(f, near, True).wait()
        leave(f, 1 - near, False).wait()
    sent(time_up, time_down)
    for t in range(frames):
        sent(*parts[t])
        sent(*blocks[t])


def on_device(
    latent, conv_cache, time_cache, norm_gain, norm_shift, conv_weight, conv_bias,
    time_weight, time_bias, up_weight, up_bias,
):
    n = lax.axis_size("rows")
    frames, row_count, wide, chan = latent.shape
    assert row_count == 1
    c_out = up_weight.shape[-1]
    pad_out = -(-c_out // 128) * 128
    width = chan // GROUPS
    member = np.arange(chan) // width
    member = jnp.asarray(member[:, None] == member[None, :], dtype=BF16)
    hbm = pl.BlockSpec(memory_space=pl.ANY)
    vmem = pl.BlockSpec(memory_space=pltpu.VMEM)
    dma = pltpu.SemaphoreType.DMA
    out = pl.pallas_call(
        functools.partial(kernel, n),
        out_shape=jax.ShapeDtypeStruct((2 * frames, 2, 2 * wide, c_out), BF16),
        in_specs=[hbm, hbm, hbm, vmem, vmem, hbm, vmem, hbm, vmem, hbm, vmem, hbm],
        out_specs=hbm,
        scratch_shapes=[
            pltpu.VMEM((frames, wide, chan), BF16),
            pltpu.VMEM((2, wide, chan), BF16),
            pltpu.VMEM((3, 2, wide, chan), BF16),
            pltpu.VMEM((3, 3 * chan, 3 * chan), BF16),
            pltpu.VMEM((3 * chan, 2 * chan), BF16),
            pltpu.VMEM((3, 3, c_out, chan), BF16),
            pltpu.VMEM(((2 + frames) * wide, 3 * chan), BF16),
            pltpu.VMEM((frames * wide, 3 * chan), F32),
            pltpu.VMEM((n, 2, chan), F32),
            pltpu.VMEM((2, frames * wide, chan), BF16),
            pltpu.VMEM((2, frames * wide, chan), BF16),
            pltpu.VMEM((3, frames * wide, chan), BF16),
            pltpu.VMEM((3, 2 * frames * wide, 3 * chan), BF16),
            pltpu.VMEM((2, 2 * pad_out, 2 * chan), BF16),
            pltpu.VMEM((2, 2, pad_out, 2 * chan), BF16),
            pltpu.VMEM((2, 2, 2 * frames * wide, pad_out), F32),
            pltpu.VMEM((pad_out // 128, 2 * wide, 128), F32),
            pltpu.VMEM((chan, chan), BF16),
            pltpu.VMEM((2 * frames, 2, 2 * wide, c_out), BF16),
            dma((6,)),
            dma((3, 9)),
            dma((n,)),
            dma((n,)),
            dma((2 + 4 * frames,)),
            dma((2 + 4 * frames,)),
            dma((2 * frames, 2)),
        ],
        compiler_params=pltpu.CompilerParams(
            collective_id=0, has_side_effects=True, vmem_limit_bytes=60000 * 1024
        ),
    )(
        latent, conv_cache, time_cache, norm_gain, norm_shift, conv_weight, conv_bias,
        time_weight.reshape(3 * chan, 2 * chan), time_bias, jnp.swapaxes(up_weight, 2, 3),
        up_bias, member,
    )
    return out


def solution(mesh):
    split = P("parts", "rows", None, None)
    return jax.shard_map(
        on_device,
        mesh=mesh,
        in_specs=(split, split, split) + (P(),) * 8,
        out_specs=split,
        check_vma=False,
    )
```

```python
import functools

import numpy as np
import jax
import jax.numpy as jnp
from jax import lax
from jax.experimental import pallas as pl
from jax.experimental.pallas import tpu as pltpu
from jax.sharding import PartitionSpec as P

GROUPS = 32
EPSILON = 1e-06
F32 = jnp.float32
BF16 = jnp.bfloat16
MESH = pl.DeviceIdType.MESH


def dot(a, b):
    return jnp.dot(a, b, preferred_element_type=F32)


def dot_turned(a, b):
    return lax.dot_general(a, b, (((1,), (1,)), ((), ())), preferred_element_type=F32)


def three_columns(value):
    wide = value.shape[0]
    column = lax.broadcasted_iota(jnp.int32, value.shape, 0)
    left = jnp.where(column == 0, 0.0, pltpu.roll(value, 1, 0))
    right = jnp.where(column == wide - 1, 0.0, pltpu.roll(value, wide - 1, 0))
    return [part.astype(BF16) for part in (left, value, right)]


def kernel(
    n, lat_hbm, cc_hbm, tc_hbm, gain_hbm, shift_hbm, cw_hbm, cb_hbm, tw_hbm, tb_hbm, uw_hbm, ub_hbm,
    member_hbm, out_hbm,
    lat, cc, tc, cw, tw, uw, xs, acc, stats, psend, precv, blk, ul, wmid, wside, uacc, rows_out, member, out, gain,
    shift, cb, tb, ub, ub_row, turn,
    in_sem, cw_sem, stat_send, stat_recv, halo_send, halo_recv, out_sem, small_sem,
):
    me = lax.axis_index("rows")
    frames, wide, chan = lat.shape
    c_out = uw.shape[2]
    pad_out = wside.shape[2]

    loads = [
        pltpu.make_async_copy(lat_hbm.at[:, 0], lat, in_sem.at[0]),
        pltpu.make_async_copy(tc_hbm.at[:, 0], tc.at[1], in_sem.at[1]),
        pltpu.make_async_copy(cc_hbm.at[:, 0], cc, in_sem.at[2]),
    ]
    loads[0].start()
    barrier = pltpu.get_barrier_semaphore()

    @pl.loop(1, n)
    def _(k):
        pl.semaphore_signal(
            barrier, inc=1, device_id={"rows": lax.rem(me + k, n)}, device_id_type=MESH
        )

    loads[1].start()
    loads[2].start()
    small = [
        pltpu.make_async_copy(src, dst, small_sem.at[i])
        for i, (src, dst) in enumerate((
            (gain_hbm, gain), (shift_hbm, shift), (cb_hbm, cb), (tb_hbm, tb), (ub_hbm, ub),
        ))
    ]
    for load in small:
        load.start()
    order = (0, 2, 1)
    taps = [[], [], []]
    for a in range(3):
        for place, b in enumerate(order):
            for c in range(3):
                copy = pltpu.make_async_copy(
                    cw_hbm.at[a, b, c],
                    cw.at[a, pl.ds(c * chan, chan), pl.ds(place * chan, chan)],
                    cw_sem.at[a, place * 3 + c],
                )
                copy.start()
                taps[a].append(copy)
    up_load = pltpu.make_async_copy(uw_hbm, uw, in_sem.at[3])
    up_load.start()
    time_load = pltpu.make_async_copy(tw_hbm, tw, in_sem.at[4])
    time_load.start()
    member_load = pltpu.make_async_copy(member_hbm, member, in_sem.at[5])
    member_load.start()

    loads[0].wait()
    signal = lat[...].astype(F32).reshape(frames * wide, chan)
    entries = float(frames * wide)
    local_sum = jnp.sum(signal, axis=0, keepdims=True)
    off = signal - local_sum / entries
    stats[me] = jnp.concatenate([local_sum, jnp.sum(off * off, axis=0, keepdims=True)], axis=0)
    pl.semaphore_wait(barrier, n - 1)

    def stat_copy(k):
        return pltpu.make_async_remote_copy(
            src_ref=stats.at[me], dst_ref=stats.at[me],
            send_sem=stat_send.at[k], recv_sem=stat_recv.at[k],
            device_id={"rows": lax.rem(me + k, n)}, device_id_type=MESH,
        )

    @pl.loop(1, n)
    def _(k):
        stat_copy(k).start()

    def to_after(src, dst, i):
        return pltpu.make_async_remote_copy(
            src_ref=src, dst_ref=dst, send_sem=halo_send.at[i], recv_sem=halo_recv.at[i],
            device_id={"rows": lax.rem(me + 1, n)}, device_id_type=MESH,
        )

    def to_before(src, dst, i):
        return pltpu.make_async_remote_copy(
            src_ref=src, dst_ref=dst, send_sem=halo_send.at[i], recv_sem=halo_recv.at[i],
            device_id={"rows": lax.rem(me + n - 1, n)}, device_id_type=MESH,
        )

    has_before = me > 0
    has_after = me < n - 1

    def exchange(up, down):
        @pl.when(has_after)
        def _():
            up.start()

        @pl.when(has_before)
        def _():
            down.start()

    def arrive(up, down):
        @pl.when(has_before)
        def _():
            up.wait_recv()

        @pl.when(has_after)
        def _():
            down.wait_recv()

    def sent(up, down):
        @pl.when(has_after)
        def _():
            up.wait_send()

        @pl.when(has_before)
        def _():
            down.wait_send()

    loads[1].wait()
    time_up = to_after(tc.at[1], tc.at[0], 0)
    time_down = to_before(tc.at[1], tc.at[2], 1)
    exchange(time_up, time_down)

    @pl.when(me == 0)
    def _():
        tc[0] = jnp.zeros_like(tc[0])
        precv[0] = jnp.zeros_like(precv[0])
        blk[0] = jnp.zeros_like(blk[0])

    @pl.when(me == n - 1)
    def _():
        tc[2] = jnp.zeros_like(tc[2])
        precv[1] = jnp.zeros_like(precv[1])
        blk[2] = jnp.zeros_like(blk[2])

    def put_three(ref, start, value):
        for i, part in enumerate(three_columns(value)):
            ref[pl.ds(start, wide), pl.ds(i * chan, chan)] = part

    loads[2].wait()
    for f in range(2):
        put_three(xs, f * wide, cc[f].astype(F32))
    for copy in taps[0]:
        copy.wait()
    acc[...] = dot(xs[pl.ds(0, 2 * wide), :], cw[0])
    for copy in taps[1]:
        copy.wait()
    acc[pl.ds(0, wide), :] += dot(xs[pl.ds(wide, wide), :], cw[1])

    for load in small:
        load.wait()
    ub_row[...] = jnp.zeros_like(ub_row)
    ub_row[:, pl.ds(0, c_out)] = ub[...][None]
    place = lax.broadcasted_iota(jnp.int32, turn.shape, 0)
    turn[...] = jnp.where(
        place == lax.broadcasted_iota(jnp.int32, turn.shape, 1), 1.0, 0.0
    ).astype(BF16)

    up_load.wait()
    wmid[...] = jnp.zeros_like(wmid)
    wside[...] = jnp.zeros_like(wside)
    w = [[uw[b, c].astype(F32) for c in range(3)] for b in range(3)]
    row_mid = ([w[1][c] + w[2][c] for c in range(3)], [w[0][c] + w[1][c] for c in range(3)])
    row_side = (w[0], w[2])
    for row in range(2):
        for dest, part in ((wmid, row_mid[row]), (wside, row_side[row])):
            pairs = ((part[0], part[1] + part[2]), (part[0] + part[1], part[2]))
            for q in range(2):
                for j in range(2):
                    value = pairs[q][j].astype(BF16)
                    lanes = pl.ds(j * chan, chan)
                    if dest is wmid:
                        dest[q, pl.ds(row * pad_out, c_out), lanes] = value
                    else:
                        dest[row, q, pl.ds(0, c_out), lanes] = value

    @pl.loop(1, n)
    def _(k):
        stat_copy(k).wait()

    total_entries = entries * n * (chan // GROUPS)
    member_load.wait()
    spread_over = member[...].astype(F32)

    def per_group(value):
        value = jnp.broadcast_to(value, (8, chan))
        got = jnp.dot(
            value, spread_over, preferred_element_type=F32, precision=lax.Precision.HIGHEST
        )
        return got[0:1]

    every = stats[...]
    sums = every[:, 0]
    center = per_group(jnp.sum(sums, axis=0, keepdims=True)) / total_entries
    gap = sums / entries - center
    squares = jnp.sum(every[:, 1] + entries * gap * gap, axis=0, keepdims=True)
    spread = per_group(squares) / total_entries
    factor = lax.rsqrt(spread + EPSILON) * gain[...][None]

    def activate(f):
        value = (lat[f].astype(F32) - center) * factor + shift[...][None]
        active = value / (1.0 + jnp.exp(-value))
        put_three(xs, (2 + f) * wide, active.astype(BF16).astype(F32))

    for copy in taps[2]:
        copy.wait()
    sides = pl.ds(0, 2 * chan)
    middle = pl.ds(2 * chan, chan)

    def frame(t):
        return pl.ds(t * wide, wide)

    parts, blocks = [], []
    for t in range(frames):
        activate(t)
        edge = acc[frame(t), sides]
        for s in range(t + 1):
            edge = edge + dot(xs[frame(2 + s), :], cw[2 + s - t, :, sides])
        psend[0, frame(t), :] = edge[:, :chan].astype(BF16)
        psend[1, frame(t), :] = edge[:, chan:].astype(BF16)
        parts.append((
            to_after(psend.at[0, frame(t)], precv.at[0, frame(t)], 2 + 2 * t),
            to_before(psend.at[1, frame(t)], precv.at[1, frame(t)], 3 + 2 * t),
        ))
        exchange(*parts[t])
    acc[frame(1), middle] += dot(xs[frame(2), :], cw[1, :, middle])
    acc[:, middle] += dot(xs[pl.ds(2 * wide, 2 * wide), :], cw[2, :, middle])
    time_load.wait()

    def temporal(row, t, keep):
        window = []
        for a in range(3):
            s = t + a
            window.append(tc[row, s] if s < 2 else blk[row, frame(s - 2), :])
        mixed = dot(jnp.concatenate(window, axis=-1), tw[...]) + tb[...][None]
        mixed = mixed.astype(BF16).astype(F32)
        if keep is not None:
            mixed = jnp.where(keep, mixed, 0.0)
        for k in range(2):
            put_three(ul.at[row], (2 * t + k) * wide, mixed[:, k * chan : (k + 1) * chan])

    def both(t):
        return pl.ds(2 * t * wide, 2 * wide)

    base = 2 + 2 * frames
    for t in range(frames):
        arrive(*parts[t])
        summed = (
            acc[frame(t), middle] + precv[0, frame(t), :].astype(F32)
            + precv[1, frame(t), :].astype(F32) + cb[...][None]
        )
        blk[1, frame(t), :] = (lat[t].astype(F32) + summed).astype(BF16)
        blocks.append((
            to_after(blk.at[1, frame(t)], blk.at[0, frame(t)], base + 2 * t),
            to_before(blk.at[1, frame(t)], blk.at[2, frame(t)], base + 2 * t + 1),
        ))
        exchange(*blocks[t])
        temporal(1, t, None)
        for q in range(2):
            got = dot_turned(ul[1, both(t), pl.ds(q * chan, 2 * chan)], wmid[q])
            for p in range(2):
                uacc[p, q, both(t), :] = got[:, p * pad_out : (p + 1) * pad_out]
    arrive(time_up, time_down)

    even = lax.rem(me, 2) == 0
    near = jnp.where(even, 1, 0)
    near_keep = jnp.where(even, has_after, has_before)
    far_keep = jnp.where(even, has_before, has_after)

    def halo(t, p, keep):
        row = 2 * p
        temporal(row, t, keep)
        for q in range(2):
            uacc[p, q, both(t), :] += dot_turned(
                ul[row, both(t), pl.ds(q * chan, 2 * chan)], wside[p, q]
            )
        for f in (2 * t, 2 * t + 1):
            for half in range(pad_out // 128):
                for q in range(2):
                    rows_out[half, pl.ds(q, wide, stride=2), :] = uacc[
                        p, q, frame(f), pl.ds(half * 128, 128)
                    ]
            rows = jnp.concatenate([rows_out[half] for half in range(pad_out // 128)], axis=-1)
            rows = (rows + ub_row[...]).astype(BF16)
            out[f, p] = dot_turned(turn[...], rows).astype(BF16)
            leave(f, p, keep is near_keep).start()

    def leave(f, p, first):
        return pltpu.make_async_copy(
            out.at[f, p], out_hbm.at[f, p], out_sem.at[f, 0 if first else 1]
        )

    for t in range(frames):
        up, down = blocks[t]

        @pl.when(even & has_after)
        def _():
            down.wait_recv()

        @pl.when(jnp.logical_not(even) & has_before)
        def _():
            up.wait_recv()

        halo(t, near, near_keep)

        @pl.when(even & has_before)
        def _():
            up.wait_recv()

        @pl.when(jnp.logical_not(even) & has_after)
        def _():
            down.wait_recv()

        halo(t, 1 - near, far_keep)
    for f in range(2 * frames):
        leave(f, near, True).wait()
        leave(f, 1 - near, False).wait()
    sent(time_up, time_down)
    for t in range(frames):
        sent(*parts[t])
        sent(*blocks[t])


def on_device(
    latent, conv_cache, time_cache, norm_gain, norm_shift, conv_weight, conv_bias,
    time_weight, time_bias, up_weight, up_bias,
):
    n = lax.axis_size("rows")
    frames, row_count, wide, chan = latent.shape
    assert row_count == 1
    c_out = up_weight.shape[-1]
    pad_out = -(-c_out // 128) * 128
    width = chan // GROUPS
    member = np.arange(chan) // width
    member = jnp.asarray(member[:, None] == member[None, :], dtype=BF16)
    hbm = pl.BlockSpec(memory_space=pl.ANY)
    dma = pltpu.SemaphoreType.DMA
    out = pl.pallas_call(
        functools.partial(kernel, n),
        out_shape=jax.ShapeDtypeStruct((2 * frames, 2, c_out, 2 * wide), BF16),
        in_specs=[hbm] * 12,
        out_specs=hbm,
        scratch_shapes=[
            pltpu.VMEM((frames, wide, chan), BF16),
            pltpu.VMEM((2, wide, chan), BF16),
            pltpu.VMEM((3, 2, wide, chan), BF16),
            pltpu.VMEM((3, 3 * chan, 3 * chan), BF16),
            pltpu.VMEM((3 * chan, 2 * chan), BF16),
            pltpu.VMEM((3, 3, c_out, chan), BF16),
            pltpu.VMEM(((2 + frames) * wide, 3 * chan), BF16),
            pltpu.VMEM((frames * wide, 3 * chan), F32),
            pltpu.VMEM((n, 2, chan), F32),
            pltpu.VMEM((2, frames * wide, chan), BF16),
            pltpu.VMEM((2, frames * wide, chan), BF16),
            pltpu.VMEM((3, frames * wide, chan), BF16),
            pltpu.VMEM((3, 2 * frames * wide, 3 * chan), BF16),
            pltpu.VMEM((2, 2 * pad_out, 2 * chan), BF16),
            pltpu.VMEM((2, 2, pad_out, 2 * chan), BF16),
            pltpu.VMEM((2, 2, 2 * frames * wide, pad_out), F32),
            pltpu.VMEM((pad_out // 128, 2 * wide, 128), F32),
            pltpu.VMEM((chan, chan), BF16),
            pltpu.VMEM((2 * frames, 2, c_out, 2 * wide), BF16),
            pltpu.VMEM((chan,), F32),
            pltpu.VMEM((chan,), F32),
            pltpu.VMEM((chan,), F32),
            pltpu.VMEM((2 * chan,), F32),
            pltpu.VMEM((c_out,), F32),
            pltpu.VMEM((1, pad_out), F32),
            pltpu.VMEM((c_out, pad_out), BF16),
            dma((6,)),
            dma((3, 9)),
            dma((n,)),
            dma((n,)),
            dma((2 + 4 * frames,)),
            dma((2 + 4 * frames,)),
            dma((2 * frames, 2)),
            dma((5,)),
        ],
        compiler_params=pltpu.CompilerParams(
            collective_id=0, has_side_effects=True, vmem_limit_bytes=60000 * 1024
        ),
    )(
        latent, conv_cache, time_cache, norm_gain, norm_shift, conv_weight, conv_bias,
        time_weight.reshape(3 * chan, 2 * chan), time_bias, jnp.swapaxes(up_weight, 2, 3),
        up_bias, member,
    )
    return jnp.swapaxes(out, 2, 3)


def solution(mesh):
    split = P("parts", "rows", None, None)
    return jax.shard_map(
        on_device,
        mesh=mesh,
        in_specs=(split, split, split) + (P(),) * 8,
        out_specs=split,
        check_vma=False,
    )
```
